32 devices in a mesh: client: 16 (over z, y, core), tp: 2 (over x).
Axes of the slice: x: 2, y: 2, z: 4, core: 2. Of those that a mesh axis runs over, the one named last changes fastest.
Arguments:
- tokens: bfloat16 [4096, 2048], P('client'), may hold values from -6 to 6
- targets: bfloat16 [4096, 2048], P('client'), may hold values from -6 to 6
- norm_gain: float32 [2048], replicated, may hold values from 0.25 to 1.75
- up_frozen: bfloat16 [2048, 7168], P('client', 'tp'), may hold values from -0.125 to 0.125
- down_frozen: bfloat16 [7168, 2048], P('tp', 'client'), may hold values from -0.0625 to 0.0625
- up_left: float32 [16, 2048], replicated, may hold values from -1 to 1
- up_right: float32 [16, 7168], P(None, 'tp'), may hold values from -0.4375 to 0.4375
- down_left: float32 [16, 7168], P(None, 'tp'), may hold values from -0.625 to 0.625
- down_right: float32 [16, 2048], replicated, may hold values from -0.0625 to 0.0625
- counts: int32 [16], P('client'), may hold values from 64 to 4096
Outputs:
- round_up_left: float32 [16, 2048], replicated
- round_up_right: float32 [16, 7168], P(None, 'tp')
- round_down_left: float32 [16, 7168], P(None, 'tp')
- round_down_right: float32 [16, 2048], replicated
The draws below stay inside these ranges and needn't reach their ends.
All inputs are finite; a program needn't handle non-finite values.
Results may differ from the reference program's by a relative error of at most 0.0089.
Values may be sent and summed in bfloat16 or wider, within the bound.
A program may use at most 128 MiB of HBM per device.

```python
import jax
import jax.numpy as jnp
from jax import lax

D = 2048
FF = 7168
RANK = 16
TOK_CLIENT = 256
STEPS = 3
CLIENTS = 16
TOKENS = 4096
N_CLIENT = 16


def set_ends(result, own_key, smallest, high):
    place = [jax.random.randint(jax.random.fold_in(own_key, axis), (), 0, length) for axis, length in enumerate(result.shape)]
    widest = result.shape.index(max(result.shape))
    next_to = place[:widest] + [(place[widest] + 1) % result.shape[widest]] + place[widest + 1:]
    return result.at[tuple(place)].set(smallest).at[tuple(next_to)].set(high)


def block_scale(stream_key, extent, cuts, smallest, high):
    gain = 1.0
    for dim, parts in cuts:
        heights = jax.random.uniform(jax.random.fold_in(jax.random.fold_in(stream_key, 6), dim), (parts,), jnp.float32, smallest / len(cuts), high / len(cuts))
        gain = gain * jnp.repeat(jnp.exp(heights), extent[dim] // parts).reshape((-1,) + (1,) * (len(extent) - 1 - dim))
    return gain


def gaussian(stream_key, extent, deviation, reach, cuts=(), dtype=jnp.bfloat16):
    gain = block_scale(stream_key, extent, cuts, -0.22, 0.18) if cuts else 1.0
    result = jax.random.normal(stream_key, extent, jnp.float32) * deviation * gain
    return jnp.minimum(jnp.maximum(result, -reach), reach).astype(dtype)


def setup_inputs(seed: int = 0) -> dict:
    splits = jax.random.split(jax.random.key(seed), 11)
    tokens = gaussian(splits[0], (TOKENS, D), 1.0, 6.0, ((0, 16),))
    targets = gaussian(splits[1], (TOKENS, D), 1.0, 6.0, ((0, 16),))
    norm_gain = jnp.clip(1.0 + 0.15 * jax.random.normal(splits[2], (D,), jnp.float32), 0.25, 1.75)
    up_frozen = gaussian(splits[3], (D, FF), D ** -0.5, 0.125, ((0, 16), (1, 2)))
    down_frozen = gaussian(splits[4], (FF, D), FF ** -0.5, 0.0625, ((0, 2), (1, 16)))
    up_left = gaussian(splits[5], (RANK, D), (max(D // 49, 1)) ** -0.5, 1.0, (), jnp.float32)
    up_right = gaussian(splits[6], (RANK, FF), 196 ** -0.5, 0.4375, ((1, 2),), jnp.float32)
    down_left = gaussian(splits[7], (RANK, FF), (max(FF // 76, 1)) ** -0.5, 0.625, ((1, 2),), jnp.float32)
    down_right = gaussian(splits[8], (RANK, D), (4 * D) ** -0.5, 0.0625, (), jnp.float32)
    counts = set_ends(jax.random.randint(splits[9], (CLIENTS,), 64, 4097), jax.random.fold_in(splits[9], 1), 64, 4096).astype(jnp.int32)
    return {"tokens": tokens, "targets": targets, "norm_gain": norm_gain, "up_frozen": up_frozen, "down_frozen": down_frozen, "up_left": up_left, "up_right": up_right, "down_left": down_left, "down_right": down_right, "counts": counts}


LEARN_RATE = 0.01
PROX_WEIGHT = 10.0
ADAPTER_SCALING = 0.5
NORM_EPS = 1e-05

def contracted_rows(left, right):
    return lax.dot_general(left, right, (((0,), (0,)), ((), ())), preferred_element_type=jnp.float32)

def contract_columns(left, right):
    return lax.dot_general(left, right, (((1,), (1,)), ((), ())), preferred_element_type=jnp.float32)

def local_train(batch, goal, norm_gain, up_frozen, down_frozen, start):
    wide = batch.astype(jnp.float32)
    scale = lax.rsqrt(lax.optimization_barrier(jnp.mean(wide * wide, axis=1, keepdims=True)) + NORM_EPS)
    normalized_input = (wide * scale * norm_gain).astype(jnp.bfloat16)
    frozen_hidden_rows = jnp.dot(normalized_input, up_frozen, preferred_element_type=jnp.float32)
    params = start
    for local_step in range(STEPS):
        up_left_b = params[0].astype(jnp.bfloat16)
        up_right_batch = params[1].astype(jnp.bfloat16)
        down_left_b = params[2].astype(jnp.bfloat16)
        down_right_batch = params[3].astype(jnp.bfloat16)
        up_low_product = contract_columns(normalized_input, up_left_b).astype(jnp.bfloat16)
        hidden_preactivation = frozen_hidden_rows + ADAPTER_SCALING * jnp.dot(up_low_product, up_right_batch, preferred_element_type=jnp.float32)
        gated_hidden = jax.nn.silu(hidden_preactivation).astype(jnp.bfloat16)
        down_low_product = contract_columns(gated_hidden, down_left_b).astype(jnp.bfloat16)
        layer_output = batch.astype(jnp.float32) + jnp.dot(gated_hidden, down_frozen, preferred_element_type=jnp.float32)
        layer_output = layer_output + ADAPTER_SCALING * jnp.dot(down_low_product, down_right_batch, preferred_element_type=jnp.float32)
        output_gradient = ((layer_output - goal.astype(jnp.float32)) / TOK_CLIENT).astype(jnp.bfloat16)
        down_low_gradient = (ADAPTER_SCALING * contract_columns(output_gradient, down_right_batch)).astype(jnp.bfloat16)
        d_gated = contract_columns(output_gradient, down_frozen) + jnp.dot(down_low_gradient, down_left_b, preferred_element_type=jnp.float32)
        sigmoid_pre = jax.nn.sigmoid(hidden_preactivation)
        hidden_gradient = (d_gated * sigmoid_pre * (1.0 + hidden_preactivation * (1.0 - sigmoid_pre))).astype(jnp.bfloat16)
        up_low_gradient = (ADAPTER_SCALING * contract_columns(hidden_gradient, up_right_batch)).astype(jnp.bfloat16)
        gradient_tree = (contracted_rows(up_low_gradient, normalized_input), ADAPTER_SCALING * contracted_rows(up_low_product, hidden_gradient), contracted_rows(down_low_gradient, gated_hidden), ADAPTER_SCALING * contracted_rows(down_low_product, output_gradient))

        def update(value, grad, anchor):
            return value - LEARN_RATE * (grad + PROX_WEIGHT * (value - anchor))
        params = jax.tree.map(update, params, gradient_tree, start)
    return params

def reference(tokens, targets, norm_gain, up_frozen, down_frozen, up_left, up_right, down_left, down_right, counts):
    token_rows = tokens.reshape(N_CLIENT, TOK_CLIENT, D)
    goal_rows = targets.reshape(N_CLIENT, TOK_CLIENT, D)
    start = (up_left, up_right, down_left, down_right)

    def visit(carry, item):
        batch, goal, weight = item
        final = local_train(batch, goal, norm_gain, up_frozen, down_frozen, start)
        scaled = weight.astype(jnp.float32)

        def accumulate(total, anchor, value):
            return total + scaled * (anchor - value)
        sums = jax.tree.map(accumulate, carry[0], start, final)
        return ((sums, carry[1] + scaled), None)
    zeros = jax.tree.map(jnp.zeros_like, start)
    (sums, total), unused = lax.scan(visit, (zeros, jnp.zeros((), jnp.float32)), (token_rows, goal_rows, counts))
    factor = LEARN_RATE * total
    return (sums[0] / factor, sums[1] / factor, sums[2] / factor, sums[3] / factor)
```

```python
import functools

import jax
import jax.numpy as jnp
from jax import lax
from jax.experimental import pallas as pl
from jax.experimental.pallas import tpu as pltpu
from jax.sharding import PartitionSpec as P

STEPS = 3
LEARN_RATE = 0.01
PROX_WEIGHT = 10.0
ADAPTER_SCALING = 0.5
NORM_EPS = 1e-05

F32 = jnp.float32
BF16 = jnp.bfloat16


def mm(a, b):
    return lax.dot_general(a, b, (((1,), (0,)), ((), ())), preferred_element_type=F32)


def mmt(a, b):
    return lax.dot_general(a, b, (((1,), (1,)), ((), ())), preferred_element_type=F32)


def update(value, grad, anchor):
    return value - LEARN_RATE * (grad + PROX_WEIGHT * (value - anchor))


def kernel(n, subs, bpd, tile, up, dnt, nx, diff, ul0, ur0, dl0, dr0, cnt,
           oul, our, odl, odr,
           w0, w1, base, dact, gate, act, ptx, prx, dout,
           ul, ur, dl, dr, ulb, drb, urb, dlb,
           lut, ldt, dldt, ldm, xtx, xrx, cntb,
           sbuf, abuf, bbuf, cbuf, rbuf,
           own_s, ring_s, ring_r, sib_s, sib_r, p_s, p_r, x_s, x_r, c_s, c_r,
           ab_s, ab_r, b_s, b_r, g_s, g_r):
    R = n // 2
    half_ring = R // 2
    me = lax.axis_index("client")
    tp = lax.axis_index("tp")
    chip = me // 2
    core = me % 2
    sib = chip * 2 + (1 - core)
    ws = (w0, w1)
    cr, ffl = w0.shape[1], w0.shape[2]
    rows = cr // 2
    piece = rows // (2 * subs)
    tok = nx.shape[1]
    n_tiles = ffl // tile

    low = chip % 2
    pos = jnp.where(low == 0, chip // 2, R - 1 - chip // 2)

    def chip_at(p):
        p = (p + 2 * R) % R
        return jnp.where(p < half_ring, 2 * p, 2 * (R - 1 - p) + 1)

    def copy(src, dst, ss, rs, client, t):
        return pltpu.make_async_remote_copy(
            src_ref=src, dst_ref=dst, send_sem=ss, recv_sem=rs,
            device_id={"client": client, "tp": t},
            device_id_type=pl.DeviceIdType.MESH)

    nbr = (chip_at(pos + 1) * 2 + core, chip_at(pos - 1) * 2 + core)

    def place(m, d, s, u, c):
        origin = chip_at(pos - s) if d == 0 else chip_at(pos + s)
        start = pl.multiple_of(c * rows + (d * subs + u) * piece, piece)
        return ws[m].at[origin, pl.ds(start, piece)]

    def ring_copy(m, d, s, u):
        ref = place(m, d, s, u, core)
        nxt = jnp.minimum(s + 1, R - 1)
        return copy(ref, ref, ring_s.at[m, d, s, u], ring_r.at[m, d, nxt, u], nbr[d], tp)

    def ring_arrived(m, d, s, u):
        ref = place(m, d, s, u, core)
        copy(ref, ref, ring_s.at[m, d, s, u], ring_r.at[m, d, s, u], nbr[d], tp).wait_recv()

    def sib_copy(m, d, s, u, c):
        ref = place(m, d, s, u, c)
        return copy(ref, ref, sib_s.at[m, d, s, u], sib_r.at[m, d, s, u], sib, tp)

    def send_own(m):
        for u in range(subs):
            for d in range(2):
                ring_copy(m, d, 0, u).start()
        for u in range(subs):
            for d in range(2):
                sib_copy(m, d, 0, u, core).start()

    def advance(m, s, forward):
        for u in range(subs):
            for d in range(2):
                ring_arrived(m, d, s, u)
                if forward:
                    ring_copy(m, d, s, u).start()
                sib_copy(m, d, s, u, core).start()

    def sib_arrived(m, dist):
        for u in range(subs):
            sib_copy(m, 0, dist, u, 1 - core).wait_recv()
            sib_copy(m, 1, (R - dist) % R, u, 1 - core).wait_recv()

    def tiles(fn, init=0):
        return lax.fori_loop(
            0, n_tiles, lambda i, c: fn(pl.ds(pl.multiple_of(i * tile, tile), tile), c), init)

    own_rows = pl.ds(pl.multiple_of(core * rows, rows), rows)
    own0 = pltpu.make_async_copy(up, w0.at[chip, own_rows], own_s.at[0])
    own1 = pltpu.make_async_copy(dnt, w1.at[chip, own_rows], own_s.at[1])
    own0.start()
    own1.start()
    own0.wait()
    send_own(0)

    cntb[me] = cnt[...]

    def cnt_copy(k):
        return copy(cntb.at[me], cntb.at[me], c_s.at[k], c_r.at[me], k, tp)

    @pl.loop(1, n)
    def _(i):
        cnt_copy((me + i) % n).start()

    base[...] = jnp.zeros_like(base)
    ul[...] = ul0[...]
    ur[...] = ur0[...]
    dl[...] = dl0[...]
    dr[...] = dr0[...]

    def add_base(dist):
        sib_arrived(0, dist)
        j = chip_at(pos - dist)

        def body(cols, c):
            base[:, cols] += mm(nx[j], w0[j, :, cols])
            return c
        tiles(body)

    def forward_piece(j):
        ptx[j] = mmt(act[...], w1[j]).astype(BF16)
        copy(ptx.at[j], prx.at[j], p_s.at[j], p_r.at[j], me, 1 - tp).start()

    def backward_piece(j):
        copy(ptx.at[j], prx.at[j], p_s.at[j], p_r.at[j], me, 1 - tp).wait_recv()
        total = ptx[j].astype(F32) + prx[j].astype(F32)
        out = diff[j] + total + ADAPTER_SCALING * mm(ldm[...], drb[j])
        grad = (out / tok).astype(BF16)
        dout[j] = grad
        dldt[...] += mmt(drb[j], grad)

        def body(cols, c):
            dact[:, cols] += mm(grad, w1[j, :, cols])
            return c
        tiles(body)

    def x_copy(k):
        return copy(xtx.at[k], xrx.at[k], x_s.at[k], x_r.at[k], me, 1 - tp)

    def begin_step():
        for j in range(R):
            ulb[j] = ul[:, j * cr:(j + 1) * cr].astype(BF16)
            drb[j] = dr[:, j * cr:(j + 1) * cr].astype(BF16)
        urb[...] = ur[...].astype(BF16)
        dlb[...] = dl[...].astype(BF16)
        low_t = lax.fori_loop(
            0, R, lambda j, c: c + mmt(ulb[j], nx[j]), jnp.zeros((ul.shape[0], tok), F32))
        lut[...] = low_t.astype(BF16)
        lu = low_t.T.astype(BF16)

        def body(cols, c):
            pre = base[:, cols] + ADAPTER_SCALING * mm(lu, urb[:, cols])
            sig = jax.nn.sigmoid(pre)
            a = (pre * sig).astype(BF16)
            act[:, cols] = a
            gate[:, cols] = sig * (1.0 + pre * (1.0 - sig))
            dact[:, cols] = jnp.zeros((tok, tile), F32)
            return c + mmt(dlb[:, cols], a)
        xtx[0] = tiles(body, jnp.zeros((ul.shape[0], tok), F32))
        x_copy(0).start()
        dldt[...] = jnp.zeros_like(dldt)

    def take_low():
        x_copy(0).wait_recv()
        total = xtx[0] + xrx[0]
        ldt[...] = total.astype(BF16)
        ldm[...] = total.T.astype(BF16)

    def end_step():
        dld = ADAPTER_SCALING * dldt[...]
        dld_t = dld.astype(BF16)
        dld_m = dld.T.astype(BF16)

        def body(cols, c):
            h = ((dact[:, cols] + mm(dld_m, dlb[:, cols])) * gate[:, cols]).astype(BF16)
            ur[:, cols] = update(ur[:, cols], ADAPTER_SCALING * mm(lut[...], h), ur0[:, cols])
            dl[:, cols] = update(dl[:, cols], mm(dld_t, act[:, cols]), dl0[:, cols])
            return c + mmt(urb[:, cols], h)
        xtx[1] = ADAPTER_SCALING * tiles(body, jnp.zeros((ul.shape[0], tok), F32))
        x_copy(1).start()
        for j in range(R):
            cols = slice(j * cr, (j + 1) * cr)
            dr[:, cols] = update(dr[:, cols], ADAPTER_SCALING * mm(ldt[...], dout[j]), dr0[:, cols])
        x_copy(1).wait_recv()
        dlu_t = (xtx[1] + xrx[1]).astype(BF16)
        for j in range(R):
            cols = slice(j * cr, (j + 1) * cr)
            ul[:, cols] = update(ul[:, cols], mm(dlu_t, nx[j]), ul0[:, cols])
        x_copy(0).wait_send()
        x_copy(1).wait_send()

        @pl.loop(0, R)
        def _(j):
            copy(ptx.at[j], prx.at[j], p_s.at[j], p_r.at[j], me, 1 - tp).wait_send()

    add_base(0)

    @pl.loop(1, half_ring)
    def _(s):
        advance(0, s, True)
    advance(0, half_ring, half_ring < R - 1)
    add_base(half_ring)

    @pl.loop(half_ring + 1, R - 1)
    def _(s):
        advance(0, s, True)
        add_base(s)
        add_base(R - s)
    own1.wait()
    send_own(1)
    advance(0, R - 1, False)
    add_base(R - 1)
    add_base(1)
    begin_step()

    def down_at(dist):
        return chip_at(pos - dist)

    sib_arrived(1, 0)
    forward_piece(chip)

    advance(1, 1, True)
    take_low()
    backward_piece(chip)

    @pl.loop(2, half_ring)
    def _(s):
        advance(1, s, True)
    advance(1, half_ring, half_ring < R - 1)
    sib_arrived(1, half_ring)
    forward_piece(down_at(half_ring))

    @pl.loop(half_ring + 1, R - 1)
    def _(s):
        advance(1, s, True)
        sib_arrived(1, s)
        forward_piece(down_at(s))
        sib_arrived(1, R - s)
        forward_piece(down_at(R - s))

        @pl.when(s == half_ring + 1)
        def _():
            backward_piece(down_at(half_ring))

        @pl.when(s > half_ring + 1)
        def _():
            backward_piece(down_at(s - 1))
            backward_piece(down_at(R - s + 1))
    advance(1, R - 1, False)
    sib_arrived(1, R - 1)
    forward_piece(down_at(R - 1))
    sib_arrived(1, 1)
    forward_piece(down_at(1))
    backward_piece(down_at(R - 2))
    backward_piece(down_at(2))
    backward_piece(down_at(R - 1))
    backward_piece(down_at(1))
    end_step()

    @pl.loop(1, STEPS)
    def _(t):
        begin_step()

        @pl.loop(0, R)
        def _(j):
            forward_piece(j)
        take_low()

        @pl.loop(0, R)
        def _(j):
            backward_piece(j)
        end_step()

    lanes = 128
    weight = cnt[0:1, 0:1]
    blocks = []
    for value, anchor, result in ((ul, ul0, oul), (ur, ur0, our), (dl, dl0, odl), (dr, dr0, odr)):
        for b in range(value.shape[1] // lanes):
            blocks.append((value, anchor, result, slice(b * lanes, (b + 1) * lanes)))
    for b in range(n * bpd):
        owner, i = divmod(b, bpd)
        c, k = divmod(owner, R)
        if b < len(blocks):
            value, anchor, _, cols = blocks[b]
            sbuf[c, k, i] = (weight * (anchor[:, cols] - value[:, cols])).astype(BF16)
        else:
            sbuf[c, k, i] = jnp.zeros(sbuf.shape[3:], BF16)
    pair = copy(sbuf.at[1 - core], abuf, ab_s.at[0], ab_r.at[0], sib, tp)
    pair.start()

    @pl.loop(1, n)
    def _(i):
        k = (me + i) % n
        copy(cntb.at[k], cntb.at[k], c_s.at[k], c_r.at[k], k, tp).wait_recv()
    total = lax.fori_loop(0, n, lambda k, c: c + cntb[k], jnp.zeros(cnt.shape, F32))
    factor = LEARN_RATE * total[0:1, 0:1]
    pair.wait_recv()

    @pl.loop(0, R)
    def _(k):
        for i in range(bpd):
            bbuf[k, i] = (sbuf[core, k, i].astype(F32) + abuf[k, i].astype(F32)).astype(BF16)

    def chip_copy(k):
        return copy(bbuf.at[k], cbuf.at[chip], b_s.at[k], b_r.at[chip], k * 2 + core, tp)

    @pl.loop(1, R)
    def _(i):
        chip_copy((chip + i) % R).start()
    cbuf[chip] = bbuf[chip]

    @pl.loop(1, R)
    def _(i):
        k = (chip + i) % R
        copy(bbuf.at[k], cbuf.at[k], b_s.at[k], b_r.at[k], k * 2 + core, tp).wait_recv()
    for i in range(bpd):
        s = lax.fori_loop(
            0, R, lambda k, c: c + cbuf[k, i].astype(F32), jnp.zeros(cbuf.shape[2:], F32))
        rbuf[core, chip, i] = (s / factor).astype(BF16)

    def back_copy(k):
        ref = rbuf.at[core, chip]
        return copy(ref, ref, g_s.at[k], g_r.at[chip], k * 2 + core, tp)

    @pl.loop(1, R)
    def _(i):
        back_copy((chip + i) % R).start()

    @pl.loop(1, R)
    def _(i):
        k = (chip + i) % R
        ref = rbuf.at[core, k]
        copy(ref, ref, g_s.at[k], g_r.at[k], k * 2 + core, tp).wait_recv()
    pair2 = copy(rbuf.at[core], rbuf.at[core], ab_s.at[1], ab_r.at[1], sib, tp)
    pair2.start()
    copy(rbuf.at[1 - core], rbuf.at[1 - core], ab_s.at[1], ab_r.at[1], sib, tp).wait_recv()
    for b in range(len(blocks)):
        owner, i = divmod(b, bpd)
        c, k = divmod(owner, R)
        _, _, result, cols = blocks[b]
        result[:, cols] = rbuf[c, k, i].astype(F32)

    pair.wait_send()
    pair2.wait_send()

    @pl.loop(1, R)
    def _(i):
        k = (chip + i) % R
        chip_copy(k).wait_send()
        back_copy(k).wait_send()

    @pl.loop(1, n)
    def _(i):
        cnt_copy((me + i) % n).wait_send()
    for m in range(2):
        for d in range(2):
            for u in range(subs):
                @pl.loop(0, R)
                def _(s):
                    sib_copy(m, d, s, u, core).wait_send()

                @pl.loop(0, R - 1)
                def _(s):
                    ring_copy(m, d, s, u).wait_send()


def per_device(n, tokens, targets, norm_gain, up_frozen, down_frozen,
               up_left, up_right, down_left, down_right, counts):
    R = n // 2
    tok, d = tokens.shape
    rank = up_left.shape[0]
    rows, ffl = up_frozen.shape
    cr = 2 * rows
    half = rows // 2
    subs = 2 if half % 32 == 0 else 1
    tile = 512 if ffl % 512 == 0 else 128
    n_blocks = 2 * (d + ffl) // 128
    bpd = -(-n_blocks // n)
    wide = tokens.astype(F32)
    scale = lax.rsqrt(jnp.mean(wide * wide, axis=1, keepdims=True) + NORM_EPS)
    nx = (wide * scale * norm_gain).astype(BF16)
    nx = nx.reshape(tok, R, cr).transpose(1, 0, 2)
    diff = (wide - targets.astype(F32)).reshape(tok, R, cr).transpose(1, 0, 2)
    cnt = jnp.broadcast_to(counts.astype(F32)[:, None], (8, 128))
    vm = pl.BlockSpec(memory_space=pltpu.VMEM)
    hbm = pl.BlockSpec(memory_space=pl.ANY)
    V = pltpu.VMEM
    dma = lambda *s: pltpu.SemaphoreType.DMA(s)
    return pl.pallas_call(
        functools.partial(kernel, n, subs, bpd, tile),
        out_shape=[jax.ShapeDtypeStruct(a.shape, F32)
                   for a in (up_left, up_right, down_left, down_right)],
        in_specs=[hbm, hbm] + [vm] * 7,
        out_specs=[vm] * 4,
        scratch_shapes=[
            V((R, cr, ffl), BF16), V((R, cr, ffl), BF16),
            V((tok, ffl), F32), V((tok, ffl), F32), V((tok, ffl), F32),
            V((tok, ffl), BF16),
            V((R, tok, cr), BF16), V((R, tok, cr), BF16), V((R, tok, cr), BF16),
            V((rank, d), F32), V((rank, ffl), F32), V((rank, ffl), F32), V((rank, d), F32),
            V((R, rank, cr), BF16), V((R, rank, cr), BF16), V((rank, ffl), BF16), V((rank, ffl), BF16),
            V((rank, tok), BF16), V((rank, tok), BF16), V((rank, tok), F32), V((tok, rank), BF16),
            V((2, rank, tok), F32), V((2, rank, tok), F32), V((n, 8, 128), F32),
            V((2, R, bpd, rank, 128), BF16), V((R, bpd, rank, 128), BF16),
            V((R, bpd, rank, 128), BF16), V((R, bpd, rank, 128), BF16),
            V((2, R, bpd, rank, 128), BF16),
            dma(2), dma(2, 2, R, subs), dma(2, 2, R, subs), dma(2, 2, R, subs), dma(2, 2, R, subs),
            dma(R), dma(R), dma(2), dma(2), dma(n), dma(n),
            dma(2), dma(2), dma(R), dma(R), dma(R), dma(R),
        ],
        compiler_params=pltpu.CompilerParams(
            vmem_limit_bytes=60 * 1024 * 1024, has_side_effects=True),
    )(up_frozen, down_frozen.T, nx, diff, up_left, up_right, down_left, down_right, cnt)


def solution(mesh):
    placed = (
        P("client", None),
        P("client", None),
        P(),
        P("client", "tp"),
        P("tp", "client"),
        P(),
        P(None, "tp"),
        P(None, "tp"),
        P(),
        P("client"),
    )
    return jax.shard_map(
        functools.partial(per_device, mesh.shape["client"]),
        mesh=mesh,
        in_specs=placed,
        out_specs=(P(), P(None, "tp"), P(None, "tp"), P()),
        check_vma=False,
    )
```

```python
import functools

import jax
import jax.numpy as jnp
from jax import lax
from jax.experimental import pallas as pl
from jax.experimental.pallas import tpu as pltpu
from jax.sharding import PartitionSpec as P

STEPS = 3
LEARN_RATE = 0.01
PROX_WEIGHT = 10.0
ADAPTER_SCALING = 0.5
NORM_EPS = 1e-05

F32 = jnp.float32
BF16 = jnp.bfloat16


def mm(a, b):
    return lax.dot_general(a, b, (((1,), (0,)), ((), ())), preferred_element_type=F32)


def mmt(a, b):
    return lax.dot_general(a, b, (((1,), (1,)), ((), ())), preferred_element_type=F32)


def update(value, grad, anchor):
    return value - LEARN_RATE * (grad + PROX_WEIGHT * (value - anchor))


def kernel(n, subs, bpd, tile, up, dnt, nx, diff, ul0, ur0, dl0, dr0, cnt,
           oul, our, odl, odr,
           w0, w1, base, dact, gate, act, ptx, prx, dout,
           ul, ur, dl, dr, ulb, drb, urb, dlb,
           lut, ldt, dldt, ldm, xtx, xrx, cntb,
           sbuf, abuf, bbuf, cbuf, rbuf,
           own_s, ring_s, ring_r, sib_s, sib_r, p_s, p_r, x_s, x_r, c_s, c_r,
           ab_s, ab_r, b_s, b_r, g_s, g_r, o_s):
    R = n // 2
    half_ring = R // 2
    me = lax.axis_index("client")
    tp = lax.axis_index("tp")
    chip = me // 2
    core = me % 2
    sib = chip * 2 + (1 - core)
    ws = (w0, w1)
    cr, ffl = w0.shape[1], w0.shape[2]
    rows = cr // 2
    piece = rows // (2 * subs)
    tok = nx.shape[1]
    n_tiles = ffl // tile

    low = chip % 2
    pos = jnp.where(low == 0, chip // 2, R - 1 - chip // 2)

    def chip_at(p):
        p = (p + 2 * R) % R
        return jnp.where(p < half_ring, 2 * p, 2 * (R - 1 - p) + 1)

    def copy(src, dst, ss, rs, client, t):
        return pltpu.make_async_remote_copy(
            src_ref=src, dst_ref=dst, send_sem=ss, recv_sem=rs,
            device_id={"client": client, "tp": t},
            device_id_type=pl.DeviceIdType.MESH)

    nbr = (chip_at(pos + 1) * 2 + core, chip_at(pos - 1) * 2 + core)

    def place(m, d, s, u, c):
        origin = chip_at(pos - s) if d == 0 else chip_at(pos + s)
        start = pl.multiple_of(c * rows + (d * subs + u) * piece, piece)
        return ws[m].at[origin, pl.ds(start, piece)]

    def ring_copy(m, d, s, u):
        ref = place(m, d, s, u, core)
        nxt = jnp.minimum(s + 1, R - 1)
        return copy(ref, ref, ring_s.at[m, d, s, u], ring_r.at[m, d, nxt, u], nbr[d], tp)

    def ring_arrived(m, d, s, u):
        ref = place(m, d, s, u, core)
        copy(ref, ref, ring_s.at[m, d, s, u], ring_r.at[m, d, s, u], nbr[d], tp).wait_recv()

    def sib_copy(m, d, s, u, c):
        ref = place(m, d, s, u, c)
        return copy(ref, ref, sib_s.at[m, d, s, u], sib_r.at[m, d, s, u], sib, tp)

    def send_own(m):
        for u in range(subs):
            for d in range(2):
                ring_copy(m, d, 0, u).start()
        for u in range(subs):
            for d in range(2):
                sib_copy(m, d, 0, u, core).start()

    def advance(m, s, forward, which=tuple(range(subs))):
        for u in which:
            for d in range(2):
                ring_arrived(m, d, s, u)
                if forward:
                    ring_copy(m, d, s, u).start()
                sib_copy(m, d, s, u, core).start()

    def sib_arrived(m, dist):
        for u in range(subs):
            sib_copy(m, 0, dist, u, 1 - core).wait_recv()
            sib_copy(m, 1, (R - dist) % R, u, 1 - core).wait_recv()

    def tiles(fn, init=0):
        return lax.fori_loop(
            0, n_tiles, lambda i, c: fn(pl.ds(pl.multiple_of(i * tile, tile), tile), c), init)

    own_rows = pl.ds(pl.multiple_of(core * rows, rows), rows)
    own0 = pltpu.make_async_copy(up, w0.at[chip, own_rows], own_s.at[0])
    own1 = pltpu.make_async_copy(dnt, w1.at[chip, own_rows], own_s.at[1])
    own0.start()
    own1.start()
    own0.wait()
    send_own(0)

    cntb[me] = cnt[...]

    def cnt_copy(k):
        return copy(cntb.at[me], cntb.at[me], c_s.at[k], c_r.at[me], k, tp)

    @pl.loop(1, n)
    def _(i):
        cnt_copy((me + i) % n).start()

    base[...] = jnp.zeros_like(base)
    ul[...] = ul0[...]
    ur[...] = ur0[...]
    dl[...] = dl0[...]
    dr[...] = dr0[...]

    def add_base(dist):
        sib_arrived(0, dist)
        j = chip_at(pos - dist)

        def body(cols, c):
            base[:, cols] += mm(nx[j], w0[j, :, cols])
            return c
        tiles(body)

    def forward_piece(j):
        ptx[j] = mmt(act[...], w1[j]).astype(BF16)
        copy(ptx.at[j], prx.at[j], p_s.at[j], p_r.at[j], me, 1 - tp).start()

    def backward_piece(j):
        copy(ptx.at[j], prx.at[j], p_s.at[j], p_r.at[j], me, 1 - tp).wait_recv()
        total = ptx[j].astype(F32) + prx[j].astype(F32)
        out = diff[j] + total + ADAPTER_SCALING * mm(ldm[...], drb[j])
        grad = (out / tok).astype(BF16)
        dout[j] = grad
        dldt[...] += mmt(drb[j], grad)

        def body(cols, c):
            dact[:, cols] += mm(grad, w1[j, :, cols])
            return c
        tiles(body)

    def x_copy(k):
        return copy(xtx.at[k], xrx.at[k], x_s.at[k], x_r.at[k], me, 1 - tp)

    def begin_step():
        for j in range(R):
            ulb[j] = ul[:, j * cr:(j + 1) * cr].astype(BF16)
            drb[j] = dr[:, j * cr:(j + 1) * cr].astype(BF16)
        urb[...] = ur[...].astype(BF16)
        dlb[...] = dl[...].astype(BF16)
        low_t = lax.fori_loop(
            0, R, lambda j, c: c + mmt(ulb[j], nx[j]), jnp.zeros((ul.shape[0], tok), F32))
        lut[...] = low_t.astype(BF16)
        lu = low_t.T.astype(BF16)

        def body(cols, c):
            pre = base[:, cols] + ADAPTER_SCALING * mm(lu, urb[:, cols])
            sig = jax.nn.sigmoid(pre)
            a = (pre * sig).astype(BF16)
            act[:, cols] = a
            gate[:, cols] = sig * (1.0 + pre * (1.0 - sig))
            dact[:, cols] = jnp.zeros((tok, tile), F32)
            return c + mmt(dlb[:, cols], a)
        xtx[0] = tiles(body, jnp.zeros((ul.shape[0], tok), F32))
        x_copy(0).start()
        dldt[...] = jnp.zeros_like(dldt)

    def take_low():
        x_copy(0).wait_recv()
        total = xtx[0] + xrx[0]
        ldt[...] = total.astype(BF16)
        ldm[...] = total.T.astype(BF16)

    def end_step():
        dld = ADAPTER_SCALING * dldt[...]
        dld_t = dld.astype(BF16)
        dld_m = dld.T.astype(BF16)

        def body(cols, c):
            h = ((dact[:, cols] + mm(dld_m, dlb[:, cols])) * gate[:, cols]).astype(BF16)
            ur[:, cols] = update(ur[:, cols], ADAPTER_SCALING * mm(lut[...], h), ur0[:, cols])
            dl[:, cols] = update(dl[:, cols], mm(dld_t, act[:, cols]), dl0[:, cols])
            return c + mmt(urb[:, cols], h)
        xtx[1] = ADAPTER_SCALING * tiles(body, jnp.zeros((ul.shape[0], tok), F32))
        x_copy(1).start()
        for j in range(R):
            cols = slice(j * cr, (j + 1) * cr)
            dr[:, cols] = update(dr[:, cols], ADAPTER_SCALING * mm(ldt[...], dout[j]), dr0[:, cols])
        x_copy(1).wait_recv()
        dlu_t = (xtx[1] + xrx[1]).astype(BF16)
        for j in range(R):
            cols = slice(j * cr, (j + 1) * cr)
            ul[:, cols] = update(ul[:, cols], mm(dlu_t, nx[j]), ul0[:, cols])
        x_copy(0).wait_send()
        x_copy(1).wait_send()

        @pl.loop(0, R)
        def _(j):
            copy(ptx.at[j], prx.at[j], p_s.at[j], p_r.at[j], me, 1 - tp).wait_send()

    first, rest = (0,), tuple(range(1, subs))

    add_base(0)

    @pl.loop(1, half_ring)
    def _(s):
        advance(0, s, True)
    advance(0, half_ring, half_ring < R - 1)

    @pl.loop(half_ring + 1, R - 1)
    def _(s):
        advance(0, s, True, first)

        @pl.when(s == half_ring + 1)
        def _():
            add_base(half_ring)

        @pl.when(s > half_ring + 1)
        def _():
            add_base(s - 1)
        advance(0, s, True, rest)

        @pl.when(s > half_ring + 1)
        def _():
            add_base(R - s + 1)
    own1.wait()
    send_own(1)
    add_base(R - 2)
    add_base(2)
    advance(0, R - 1, False)
    add_base(R - 1)
    add_base(1)
    advance(1, 1, True, first)
    begin_step()
    advance(1, 1, True, rest)

    def down_at(dist):
        return chip_at(pos - dist)

    sib_arrived(1, 0)
    forward_piece(chip)

    take_low()
    backward_piece(chip)

    @pl.loop(2, half_ring)
    def _(s):
        advance(1, s, True)
    advance(1, half_ring, half_ring < R - 1)
    sib_arrived(1, half_ring)
    forward_piece(down_at(half_ring))

    @pl.loop(half_ring + 1, R - 1)
    def _(s):
        advance(1, s, True, first)

        @pl.when(s == half_ring + 1)
        def _():
            backward_piece(down_at(half_ring))

        @pl.when(s > half_ring + 1)
        def _():
            backward_piece(down_at(s - 1))
            backward_piece(down_at(R - s + 1))
        advance(1, s, True, rest)
        sib_arrived(1, s)
        forward_piece(down_at(s))
        sib_arrived(1, R - s)
        forward_piece(down_at(R - s))
    advance(1, R - 1, False, first)
    backward_piece(down_at(R - 2))
    backward_piece(down_at(2))
    advance(1, R - 1, False, rest)
    sib_arrived(1, R - 1)
    forward_piece(down_at(R - 1))
    sib_arrived(1, 1)
    forward_piece(down_at(1))
    backward_piece(down_at(R - 1))
    backward_piece(down_at(1))
    end_step()

    @pl.loop(1, STEPS)
    def _(t):
        begin_step()

        @pl.loop(0, R)
        def _(j):
            forward_piece(j)
        take_low()

        @pl.loop(0, R)
        def _(j):
            backward_piece(j)
        end_step()

    lanes = 128
    weight = cnt[0:1, 0:1]
    blocks = []
    for value, anchor, result in ((ul, ul0, oul), (ur, ur0, our), (dl, dl0, odl), (dr, dr0, odr)):
        for b in range(value.shape[1] // lanes):
            blocks.append((value, anchor, result, slice(b * lanes, (b + 1) * lanes)))
    for b in range(n * bpd):
        owner, i = divmod(b, bpd)
        c, k = divmod(owner, R)
        if b < len(blocks):
            value, anchor, _, cols = blocks[b]
            sbuf[c, k, i] = (weight * (anchor[:, cols] - value[:, cols])).astype(BF16)
        else:
            sbuf[c, k, i] = jnp.zeros(sbuf.shape[3:], BF16)
    pair = copy(sbuf.at[1 - core], abuf, ab_s.at[0], ab_r.at[0], sib, tp)
    pair.start()

    @pl.loop(1, n)
    def _(i):
        k = (me + i) % n
        copy(cntb.at[k], cntb.at[k], c_s.at[k], c_r.at[k], k, tp).wait_recv()
    total = lax.fori_loop(0, n, lambda k, c: c + cntb[k], jnp.zeros(cnt.shape, F32))
    factor = LEARN_RATE * total[0:1, 0:1]
    pair.wait_recv()

    @pl.loop(0, R)
    def _(k):
        for i in range(bpd):
            bbuf[k, i] = (sbuf[core, k, i].astype(F32) + abuf[k, i].astype(F32)).astype(BF16)

    def chip_copy(k):
        return copy(bbuf.at[k], cbuf.at[chip], b_s.at[k], b_r.at[chip], k * 2 + core, tp)

    @pl.loop(1, R)
    def _(i):
        chip_copy((chip + i) % R).start()
    cbuf[chip] = bbuf[chip]

    @pl.loop(1, R)
    def _(i):
        k = (chip + i) % R
        copy(bbuf.at[k], cbuf.at[k], b_s.at[k], b_r.at[k], k * 2 + core, tp).wait_recv()
    for i in range(bpd):
        s = lax.fori_loop(
            0, R, lambda k, c: c + cbuf[k, i].astype(F32), jnp.zeros(cbuf.shape[2:], F32))
        rbuf[core, chip, i] = (s / factor).astype(BF16)

    def back_copy(k):
        ref = rbuf.at[core, chip]
        return copy(ref, ref, g_s.at[k], g_r.at[chip], k * 2 + core, tp)

    @pl.loop(1, R)
    def _(i):
        back_copy((chip + i) % R).start()

    @pl.loop(1, R)
    def _(i):
        k = (chip + i) % R
        ref = rbuf.at[core, k]
        copy(ref, ref, g_s.at[k], g_r.at[k], k * 2 + core, tp).wait_recv()
    pair2 = copy(rbuf.at[core], rbuf.at[core], ab_s.at[1], ab_r.at[1], sib, tp)
    pair2.start()
    copy(rbuf.at[1 - core], rbuf.at[1 - core], ab_s.at[1], ab_r.at[1], sib, tp).wait_recv()
    for b in range(len(blocks)):
        owner, i = divmod(b, bpd)
        c, k = divmod(owner, R)
        value, _, _, cols = blocks[b]
        value[:, cols] = rbuf[c, k, i].astype(F32)
    outs = [pltpu.make_async_copy(v, o, o_s.at[i])
            for i, (v, o) in enumerate(((ul, oul), (ur, our), (dl, odl), (dr, odr)))]
    for o in outs:
        o.start()

    pair.wait_send()
    pair2.wait_send()

    @pl.loop(1, R)
    def _(i):
        k = (chip + i) % R
        chip_copy(k).wait_send()
        back_copy(k).wait_send()

    @pl.loop(1, n)
    def _(i):
        cnt_copy((me + i) % n).wait_send()
    for m in range(2):
        for d in range(2):
            for u in range(subs):
                @pl.loop(0, R)
                def _(s):
                    sib_copy(m, d, s, u, core).wait_send()

                @pl.loop(0, R - 1)
                def _(s):
                    ring_copy(m, d, s, u).wait_send()
    for o in outs:
        o.wait()


def per_device(n, tokens, targets, norm_gain, up_frozen, down_frozen,
               up_left, up_right, down_left, down_right, counts):
    R = n // 2
    tok, d = tokens.shape
    rank = up_left.shape[0]
    rows, ffl = up_frozen.shape
    cr = 2 * rows
    half = rows // 2
    subs = 2 if half % 32 == 0 else 1
    tile = 512 if ffl % 512 == 0 else 128
    n_blocks = 2 * (d + ffl) // 128
    bpd = -(-n_blocks // n)
    wide = tokens.astype(F32)
    scale = lax.rsqrt(jnp.mean(wide * wide, axis=1, keepdims=True) + NORM_EPS)
    nx = (wide * scale * norm_gain).astype(BF16)
    nx = nx.reshape(tok, R, cr).transpose(1, 0, 2)
    diff = (wide - targets.astype(F32)).reshape(tok, R, cr).transpose(1, 0, 2)
    cnt = jnp.broadcast_to(counts.astype(F32)[:, None], (8, 128))
    vm = pl.BlockSpec(memory_space=pltpu.VMEM)
    hbm = pl.BlockSpec(memory_space=pl.ANY)
    V = pltpu.VMEM
    dma = lambda *s: pltpu.SemaphoreType.DMA(s)
    return pl.pallas_call(
        functools.partial(kernel, n, subs, bpd, tile),
        out_shape=[jax.ShapeDtypeStruct(a.shape, F32)
                   for a in (up_left, up_right, down_left, down_right)],
        in_specs=[hbm, hbm] + [vm] * 7,
        out_specs=[pl.BlockSpec(memory_space=pltpu.HBM)] * 4,
        scratch_shapes=[
            V((R, cr, ffl), BF16), V((R, cr, ffl), BF16),
            V((tok, ffl), F32), V((tok, ffl), F32), V((tok, ffl), F32),
            V((tok, ffl), BF16),
            V((R, tok, cr), BF16), V((R, tok, cr), BF16), V((R, tok, cr), BF16),
            V((rank, d), F32), V((rank, ffl), F32), V((rank, ffl), F32), V((rank, d), F32),
            V((R, rank, cr), BF16), V((R, rank, cr), BF16), V((rank, ffl), BF16), V((rank, ffl), BF16),
            V((rank, tok), BF16), V((rank, tok), BF16), V((rank, tok), F32), V((tok, rank), BF16),
            V((2, rank, tok), F32), V((2, rank, tok), F32), V((n, 8, 128), F32),
            V((2, R, bpd, rank, 128), BF16), V((R, bpd, rank, 128), BF16),
            V((R, bpd, rank, 128), BF16), V((R, bpd, rank, 128), BF16),
            V((2, R, bpd, rank, 128), BF16),
            dma(2), dma(2, 2, R, subs), dma(2, 2, R, subs), dma(2, 2, R, subs), dma(2, 2, R, subs),
            dma(R), dma(R), dma(2), dma(2), dma(n), dma(n),
            dma(2), dma(2), dma(R), dma(R), dma(R), dma(R), dma(4),
        ],
        compiler_params=pltpu.CompilerParams(
            vmem_limit_bytes=60 * 1024 * 1024, has_side_effects=True),
    )(up_frozen, down_frozen.T, nx, diff, up_left, up_right, down_left, down_right, cnt)


def solution(mesh):
    placed = (
        P("client", None),
        P("client", None),
        P(),
        P("client", "tp"),
        P("tp", "client"),
        P(),
        P(None, "tp"),
        P(None, "tp"),
        P(),
        P("client"),
    )
    return jax.shard_map(
        functools.partial(per_device, mesh.shape["client"]),
        mesh=mesh,
        in_specs=placed,
        out_specs=(P(), P(None, "tp"), P(None, "tp"), P()),
        check_vma=False,
    )
```
